256 devices in a mesh: turn: 8 (over y, core), blk: 16 (over x_lo, z), strip: 2 (over x_hi).
Axes of the slice: x: 4 (x_hi: 2, x_lo: 2; x = x_hi * 2 + x_lo), y: 4, z: 8, core: 2. Of those that a mesh axis runs over, the one named last changes fastest.
Arguments:
- echoes: bfloat16 [2, 2048, 32768], P(None, 'blk', ('turn', 'strip')), may hold values from -6 to 6
- filters: bfloat16 [2, 32, 32768], P(None, 'blk'), may hold values from -6 to 6
- slab_index: int32 [2048], P(('blk', 'turn')), may hold values from 0 to 31
- shifts: int32 [2048], P(('blk', 'turn')), may hold values from 0 to 32767
Outputs:
- focused: float32 [2, 2048, 32768], P(None, ('blk', 'turn'), 'strip')
The draws below stay inside these ranges and needn't reach their ends.
All inputs are finite; a program needn't handle non-finite values.
Results may differ from the reference program's by a relative error of at most 0.0003.
Values may be sent and summed in bfloat16 or wider, within the bound.
A program may use at most 128 MiB of HBM per device.

```python
import jax
import jax.numpy as jnp
from jax import lax

NA = 32768
NR = 2048
NS = 32


def plant(entries, stream_key, smallest, largest):
    dims = entries.shape
    place = [jax.random.randint(jax.random.fold_in(stream_key, axis), (), 0, dims[axis]) for axis in range(len(dims))]
    entries = entries.at[tuple(place)].set(smallest)
    longest = dims.index(max(dims))
    place[longest] = (place[longest] + 1) % dims[longest]
    return entries.at[tuple(place)].set(largest)


def block_scale(own_key, extent, split, smallest, high):
    loudness, own = 1.0, jax.random.fold_in(own_key, 6)
    for dim, blocks in split:
        steps = jnp.exp(jax.random.uniform(jax.random.fold_in(own, dim), (blocks,), jnp.float32, smallest / len(split), high / len(split)))
        loudness = loudness * jnp.repeat(steps, extent[dim] // blocks).reshape([-1 if axis == dim else 1 for axis in range(len(extent))])
    return loudness


def scatter_about(rng, shape, scale, limit, split=(), kind=jnp.bfloat16):
    values = jax.random.normal(rng, shape, jnp.float32) * scale
    if len(split) > 0:
        values = block_scale(rng, shape, split, -0.22, 0.18) * values
    return jnp.clip(values, min=-limit, max=limit).astype(kind)


def setup_inputs(seed: int = 0) -> dict:
    key_of = jax.random.split(jax.random.key(seed), 5)
    echoes = scatter_about(key_of[0], (2, NR, NA), 1.0, 6.0, ((1, 16), (2, 16)))
    filters = scatter_about(key_of[1], (2, NS, NA), 1.0, 6.0, ((1, 16),))
    slab_index = plant(jax.random.randint(key_of[2], (NR,), 0, NS), jax.random.fold_in(key_of[2], 1), 0, NS - 1).astype(jnp.int32)
    shifts = plant(jax.random.randint(key_of[3], (NR,), 0, NA), jax.random.fold_in(key_of[3], 1), 0, NA - 1).astype(jnp.int32)
    return dict(echoes=echoes, filters=filters, slab_index=slab_index, shifts=shifts)


def reference(echoes, filters, slab_index, shifts):
    signal = lax.complex(echoes[0].astype(jnp.float32), echoes[1].astype(jnp.float32))
    spectrum = jnp.fft.fft(signal, axis=1)
    chosen = lax.complex(filters[0][slab_index].astype(jnp.float32), filters[1][slab_index].astype(jnp.float32))
    image = jnp.fft.ifft(spectrum * chosen, axis=1)
    positions = (jnp.arange(NA, dtype=jnp.int32)[None, :] - shifts[:, None].astype(jnp.int32)) % NA
    rolled = jnp.take_along_axis(image, positions, axis=1)
    return jnp.stack([jnp.real(rolled), jnp.imag(rolled)]).astype(jnp.float32)
```

```python
import functools
import math

import numpy as np
import jax
import jax.numpy as jnp
from jax import lax
from jax.experimental import pallas as pl
from jax.experimental.pallas import tpu as pltpu
from jax.sharding import PartitionSpec as P

N = 32768
f32, bf16 = jnp.float32, jnp.bfloat16
MESH = pl.DeviceIdType.MESH

def cis(phase, length, sign):
    ang = (np.asarray(phase, np.int64) % length).astype(np.float64) * (2 * np.pi / length)
    return np.cos(ang), sign * np.sin(ang)

def halves(mat):
    hi = mat.astype(np.float32).astype(bf16)
    lo = (mat - hi.astype(np.float64)).astype(np.float32).astype(bf16)
    return hi, lo

def tables():
    lane = np.arange(128)
    c, s = cis(np.outer(lane, lane), 128, -1)
    fwd = np.block([[c, s], [-s, c]])
    inv = np.block([[c, -s], [s, c]]) / N
    mats = np.stack([*halves(fwd), *halves(inv)])
    tile = np.arange(256)
    tw = np.stack(cis(np.outer(tile, lane), N, -1)).astype(np.float32)
    ij = np.outer(np.arange(16), np.arange(16)).reshape(256, 1) * np.ones((1, 128), np.int64)
    ct = np.stack(cis(ij, 256, -1)).astype(np.float32)
    return mats, np.concatenate([tw, ct])

R2 = math.sqrt(0.5)
C1, S1 = math.cos(math.pi / 8), math.sin(math.pi / 8)

def cadd(a, b): return (a[0] + b[0], a[1] + b[1])
def csub(a, b): return (a[0] - b[0], a[1] - b[1])

def turn16(a, p, sign):
    p = (sign * p) % 16
    q, r = divmod(p, 4)
    x, y = a
    if r == 2:
        x, y = ((x - y) * R2, (x + y) * R2)
    elif r:
        c, s = (C1, S1) if r == 1 else (S1, C1)
        x, y = (x * c - y * s, x * s + y * c)
    return [(x, y), (-y, x), (-x, -y), (y, -x)][q]

def fold4(a, b, c, d, sign):
    e, f, g, h = cadd(a, c), csub(a, c), cadd(b, d), csub(b, d)
    if sign > 0:
        t, u = (f[0] - h[1], f[1] + h[0]), (f[0] + h[1], f[1] - h[0])
    else:
        t, u = (f[0] + h[1], f[1] - h[0]), (f[0] - h[1], f[1] + h[0])
    return cadd(e, g), t, csub(e, g), u

def dft16(v, sign):
    cols = [fold4(v[b], v[b + 4], v[b + 8], v[b + 12], sign) for b in range(4)]
    out = [None] * 16
    for a in range(4):
        o = fold4(*[turn16(cols[b][a], a * b, sign) for b in range(4)], sign)
        for c in range(4):
            out[a + 4 * c] = o[c]
    return out

def dft8(v, sign):
    even = fold4(v[0], v[2], v[4], v[6], sign)
    odd = fold4(v[1], v[3], v[5], v[7], sign)
    odd = [turn16(o, 2 * i, sign) for i, o in enumerate(odd)]
    return [cadd(e, o) for e, o in zip(even, odd)] + [csub(e, o) for e, o in zip(even, odd)]

def half16(v, sign, flip):
    even = dft8(v[0::2], sign)
    odd = dft8([(flip * a, flip * b) for a, b in v[1::2]], sign)
    return [cadd(e, turn16(o, i, sign)) for i, (e, o) in enumerate(zip(even, odd))]

def cmul(a, c, s): return (a[0] * c - a[1] * s, a[0] * s + a[1] * c)
def cmulc(a, c, s): return (a[0] * c + a[1] * s, a[1] * c - a[0] * s)

def split(x):
    hi = x.astype(bf16)
    return hi, (x - hi.astype(f32)).astype(bf16)

def stage_j(xs, y, tab):
    def body(m1, _):
        lanes = pl.ds(pl.multiple_of(m1 * 128, 128), 128)
        v = [(xs[j, 0, :, lanes].astype(f32), xs[j, 1, :, lanes].astype(f32)) for j in range(16)]
        for k0, a in enumerate(dft16(v, -1)):
            if k0:
                row = pl.ds(m1 * 16 + k0, 1)
                a = cmul(a, tab[2, row, :], tab[3, row, :])
            y[0, k0 * 16 + m1], y[1, k0 * 16 + m1] = a
        return 0
    lax.fori_loop(0, 16, body, 0)

def put_pair(hi_ref, lo_ref, row, a, b):
    rows = pl.ds(pl.multiple_of(row, 16), 16)
    for part, lanes in ((0, slice(0, 128)), (1, slice(128, 256))):
        hi, lo = split(jnp.concatenate([a[part], b[part]], axis=0))
        hi_ref[rows, lanes] = hi
        lo_ref[rows, lanes] = lo

def stage_m(y, hi_ref, lo_ref, tab):
    def body(k0, _):
        out = dft16([(y[0, k0 * 16 + m1], y[1, k0 * 16 + m1]) for m1 in range(16)], -1)
        out = [cmul(a, tab[0, pl.ds(k0 + 16 * k1, 1), :], tab[1, pl.ds(k0 + 16 * k1, 1), :]) for k1, a in enumerate(out)]
        for k1 in range(0, 16, 2):
            put_pair(hi_ref, lo_ref, k0 * 128 + k1 * 8, out[k1], out[k1 + 1])
        return 0
    lax.fori_loop(0, 16, body, 0)

def dot3(hi, lo, whi, wlo):
    d = functools.partial(jnp.dot, preferred_element_type=f32)
    return d(hi, whi) + d(lo, whi) + d(hi, wlo)

def mid(hi_ref, lo_ref, resp, mats, chunk=512):
    def body(i, _):
        rows = pl.ds(pl.multiple_of(i * chunk, chunk), chunk)
        s = dot3(hi_ref[rows, :], lo_ref[rows, :], mats[0], mats[1])
        p = cmul((s[:, :128], s[:, 128:]), resp[0, rows, :], resp[1, rows, :])
        for part, lanes in ((0, slice(0, 128)), (1, slice(128, 256))):
            hi, lo = split(p[part])
            hi_ref[rows, lanes] = hi
            lo_ref[rows, lanes] = lo
        return 0
    lax.fori_loop(0, 2048 // chunk, body, 0)

def back(hi_ref, lo_ref, q, mats, chunk=512):
    def body(i, _):
        rows = pl.ds(pl.multiple_of(i * chunk, chunk), chunk)
        q[rows, :] = dot3(hi_ref[rows, :], lo_ref[rows, :], mats[2], mats[3])
        return 0
    lax.fori_loop(0, 2048 // chunk, body, 0)

def stage_k1(q, y, tab):
    def body(k0, _):
        v = []
        for k1 in range(16):
            rows = pl.ds(pl.multiple_of(k0 * 128 + k1 * 8, 8), 8)
            row = pl.ds(k0 + 16 * k1, 1)
            v.append(cmulc((q[rows, 0:128], q[rows, 128:256]), tab[0, row, :], tab[1, row, :]))
        for m1, a in enumerate(dft16(v, 1)):
            y[0, k0 * 16 + m1], y[1, k0 * 16 + m1] = a
        return 0
    lax.fori_loop(0, 16, body, 0)

def stage_k0(y, out, tab, flip, g):
    def body(m1, _):
        v = []
        for k0 in range(16):
            a = (y[0, k0 * 16 + m1], y[1, k0 * 16 + m1])
            if k0:
                row = pl.ds(m1 * 16 + k0, 1)
                a = cmulc(a, tab[2, row, :], tab[3, row, :])
            v.append(a)
        for j, a in enumerate(half16(v, 1, flip)):
            lanes = pl.ds(pl.multiple_of(j * 2048 + m1 * 128, 128), 128)
            out[0, 8 * g:8 * g + 8, lanes], out[1, 8 * g:8 * g + 8, lanes] = a
        return 0
    lax.fori_loop(0, 16, body, 0)

def phase(idx):
    idx = (idx & (N - 1))
    idx = jnp.where(idx >= N // 2, idx - N, idx)
    ang = idx.astype(f32) * (2 * math.pi / N)
    return jnp.cos(ang), -jnp.sin(ang)

def response(bank, slabs, shifts, resp):
    sub = lax.broadcasted_iota(jnp.int32, (8, 128), 0)
    lane = lax.broadcasted_iota(jnp.int32, (8, 128), 1)
    for g in range(2):
        def body(r, _):
            sl = slabs[8 * g + r]
            sh = shifts[8 * g + r]
            e = [phase((16 * (sub + 8 * h) + 256 * lane) * sh) for h in range(2)]
            w = phase(jnp.full((8, 128), 1, jnp.int32) * sh)
            for i in range(16):
                hr = bank[0, sl, 16 * i:16 * i + 16, :].astype(f32)
                hi = bank[1, sl, 16 * i:16 * i + 16, :].astype(f32)
                for h in range(2):
                    o = cmul((hr[8 * h:8 * h + 8], hi[8 * h:8 * h + 8]), *e[h])
                    rows = pl.ds((16 * i + 8 * h) * 8 + r, 8, stride=8)
                    resp[g, 0, rows, :] = o[0]
                    resp[g, 1, rows, :] = o[1]
                if i < 15:
                    e = [cmul(x, *w) for x in e]
            return 0
        lax.fori_loop(0, 8, body, 0)


def place_filters(raw, lines, turned, bank, part, chunk):
    def spread(i, _):
        lanes = pl.ds(pl.multiple_of(i * 2048, 2048), 2048)
        block = raw[:, lanes].astype(f32)
        for t in range(16):
            for slab in range(2):
                lines[slab, pl.ds(i * 16 + t, 1), :] = block[slab:slab + 1, 128 * t:128 * t + 128]
        return 0
    lax.fori_loop(0, 16, spread, 0)
    for slab in range(2):
        for h in range(2):
            flat = jnp.transpose(lines[slab, pl.ds(h, 128, stride=2), :])
            for b in range(8):
                turned[slab, pl.ds(8 * h + b, 16, stride=16), :] = flat[16 * b:16 * b + 16]
        bank[part, 2 * chunk + slab] = turned[slab].astype(bf16)


def kernel(
    echoes, filters, slabs, shifts, mats_h, tab_h, out_h,
    xs, est, bank, raw, lines, turned, mats, tab, y, ahi, alo, q, resp, out,
    loc, es, er, fs, fr, zs, zr, cs, cr,
):
    t, b, s = (lax.axis_index(n) for n in ("turn", "blk", "strip"))
    yy, core = t // 2, t % 2
    xlo, z = b // 8, b % 8
    xx = 2 * s + xlo

    def at_y(dy, dc):
        return (((yy + dy) % 4) * 2 + (core + dc) % 2, b, s)

    def at_x(d):
        x = (xx + d) % 4
        return (t, (x % 2) * 8 + z, x // 2)

    def at_z(d):
        return (t, xlo * 8 + (z + d) % 8, s)

    mate, twin = at_y(0, 1), (t, b, 1 - s)
    peers = [at_y(dy, dc) for dy, dc in ((0, 1), (1, 0), (3, 0), (1, 1), (3, 1), (2, 0), (2, 1))]

    barrier = pltpu.get_barrier_semaphore()
    known = peers + [twin, at_x(1), at_x(3), at_z(1), at_z(7)]
    for d in known:
        pl.semaphore_signal(barrier, inc=1, device_id=d, device_id_type=MESH)

    mine = 2 * t + s
    local = [
        pltpu.make_async_copy(filters.at[core], raw, loc.at[0]),
        pltpu.make_async_copy(echoes, est, loc.at[1]),
        pltpu.make_async_copy(echoes.at[:, t, 0], xs.at[0, mine], loc.at[2]),
        pltpu.make_async_copy(echoes.at[:, t, 1], xs.at[1, mine], loc.at[3]),
        pltpu.make_async_copy(mats_h, mats, loc.at[4]),
        pltpu.make_async_copy(tab_h, tab, loc.at[5]),
    ]
    for c in local:
        c.start()
    local[0].wait()
    place_filters(raw, lines, turned, bank, core, b)
    for c in local[1:]:
        c.wait()
    pl.semaphore_wait(barrier, len(known))

    sent = []

    def send(src, dst, ssem, rsem, device):
        c = pltpu.make_async_remote_copy(
            src, dst, ssem, rsem, device_id=device, device_id_type=MESH
        )
        c.start()
        sent.append(c)

    def arrived(ref, ssem, rsem):
        pltpu.make_async_remote_copy(
            ref, ref, ssem, rsem, device_id=twin, device_id_type=MESH
        ).wait_recv()

    def slot(device):
        return 2 * device[0] + s

    def forward(g, j):
        ref = xs.at[g, j]
        send(ref, ref, es.at[g, j], er.at[g, j], twin)

    def echo(g, device):
        j = slot(device)
        arrived(xs.at[g, j], es.at[g, j], er.at[g, j])
        forward(g, j)

    def chunk(u, d):
        side = xlo if u == 0 else 1 - xlo
        return 2 * (side * 8 + (z + d) % 8)

    def piece(u, d, hop, way):
        start = chunk(u, d)
        if hop == 4:
            return bank.at[core, pl.ds(start + way, 1)]
        return bank.at[core, pl.ds(start, 2)]

    def over_z(u, hop, way):
        d = (1 - hop) if way == 0 else (hop - 1)
        ref = piece(u, d % 8, hop, way)
        send(ref, ref, zs.at[way, hop - 1, u], zr.at[way, hop - 1, u], at_z(1 if way == 0 else 7))

    def over_core(ref, n):
        send(ref, ref, cs.at[n], cr.at[n], mate)

    def relay(u, hop):
        for way in range(2):
            d = (-hop if way == 0 else hop) % 8
            ref = piece(u, d, hop, way)
            arrived(ref, zs.at[way, hop - 1, u], zr.at[way, hop - 1, u])
            if hop < 4:
                over_z(u, hop + 1, way)
            n = 2 + (hop - 1) * 4 + 2 * u + way
            over_core(ref, n)

    own = bank.at[core, pl.ds(2 * b, 2)]
    for i, d in ((0, 1), (1, 3)):
        ref = bank.at[core, pl.ds(2 * b + i, 1)]
        send(ref, ref, fs.at[i], fr.at[i], at_x(d))
    over_z(0, 1, 0)
    over_z(0, 1, 1)
    for g in range(2):
        for k, d in enumerate(peers):
            send(est.at[:, d[0], g], xs.at[g, mine], loc.at[8 + 8 * g + k], er.at[g, mine], d)
        forward(g, mine)
    over_core(own, 0)

    echo(0, peers[0])
    for i in range(2):
        arrived(bank.at[core, pl.ds(chunk(1, 0) + i, 1)], fs.at[i], fr.at[i])
    over_z(1, 1, 0)
    over_z(1, 1, 1)
    over_core(bank.at[core, pl.ds(chunk(1, 0), 2)], 1)
    for d in peers[1:5]:
        echo(0, d)
    relay(0, 1)
    for d in peers[5:]:
        echo(0, d)
    relay(1, 1)
    echo(1, peers[0])
    echo(1, peers[1])
    echo(1, peers[2])
    relay(0, 2)
    echo(1, peers[3])
    echo(1, peers[4])
    relay(1, 2)
    echo(1, peers[5])
    echo(1, peers[6])
    relay(0, 3)
    relay(1, 3)
    relay(0, 4)
    relay(1, 4)
    for g in range(2):
        for k in range(8):
            j = 2 * k + 1 - s
            arrived(xs.at[g, j], es.at[g, j], er.at[g, j])
    for n in range(18):
        if n < 2:
            ref = bank.at[1 - core, pl.ds(chunk(n, 0), 2)]
        else:
            hop, u, way = (n - 2) // 4 + 1, (n - 2) // 2 % 2, n % 2
            d = (-hop if way == 0 else hop) % 8
            start = chunk(u, d)
            ref = bank.at[1 - core, pl.ds(start + way, 1) if hop == 4 else pl.ds(start, 2)]
        arrived(ref, cs.at[n], cr.at[n])

    flip = 1.0 - 2.0 * s.astype(f32)
    response(bank, slabs, shifts, resp)
    for g in range(2):
        stage_j(xs.at[g], y, tab)
        stage_m(y, ahi, alo, tab)
        mid(ahi, alo, resp.at[g], mats)
        back(ahi, alo, q, mats)
        stage_k1(q, y, tab)
        stage_k0(y, out, tab, flip, g)
    result = pltpu.make_async_copy(out, out_h, loc.at[6])
    result.start()
    for c in sent:
        c.wait_send()
    result.wait()


def per_device(echoes, filters, slab_index, shifts):
    mats, tab = tables()
    hbm = pl.BlockSpec(memory_space=pl.ANY)
    smem = pl.BlockSpec(memory_space=pltpu.SMEM)
    dma = pltpu.SemaphoreType.DMA
    return pl.pallas_call(
        kernel,
        out_shape=jax.ShapeDtypeStruct((2, 16, N // 2), f32),
        in_specs=[hbm, hbm, smem, smem, hbm, hbm],
        out_specs=hbm,
        scratch_shapes=[
            pltpu.VMEM((2, 16, 2, 8, 2048), bf16),
            pltpu.VMEM((2, 8, 2, 8, 2048), bf16),
            pltpu.VMEM((2, 32, 256, 128), bf16),
            pltpu.VMEM((2, N), bf16),
            pltpu.VMEM((2, 256, 128), f32),
            pltpu.VMEM((2, 256, 128), f32),
            pltpu.VMEM((4, 256, 256), bf16),
            pltpu.VMEM((4, 256, 128), f32),
            pltpu.VMEM((2, 256, 8, 128), f32),
            pltpu.VMEM((2048, 256), bf16),
            pltpu.VMEM((2048, 256), bf16),
            pltpu.VMEM((2048, 256), f32),
            pltpu.VMEM((2, 2, 2048, 128), f32),
            pltpu.VMEM((2, 16, N // 2), f32),
            dma((24,)),
            dma((2, 16)),
            dma((2, 16)),
            dma((2,)),
            dma((2,)),
            dma((2, 4, 2)),
            dma((2, 4, 2)),
            dma((18,)),
            dma((18,)),
        ],
        compiler_params=pltpu.CompilerParams(
            collective_id=0, has_side_effects=True, vmem_limit_bytes=60 << 20
        ),
    )(
        echoes.reshape(2, 8, 2, 8, 2048), filters, slab_index, shifts,
        jnp.asarray(mats), jnp.asarray(tab),
    )


def solution(mesh):
    in_specs = (
        P(None, "blk", ("turn", "strip")),
        P(None, "blk", None),
        P(("blk", "turn")),
        P(("blk", "turn")),
    )
    out_specs = P(None, ("blk", "turn"), "strip")
    return jax.shard_map(
        per_device, mesh=mesh, in_specs=in_specs, out_specs=out_specs, check_vma=False
    )
```

```python
import functools
import math

import numpy as np
import jax
import jax.numpy as jnp
from jax import lax
from jax.experimental import pallas as pl
from jax.experimental.pallas import tpu as pltpu
from jax.sharding import PartitionSpec as P

N = 32768
f32, bf16 = jnp.float32, jnp.bfloat16
MESH = pl.DeviceIdType.MESH

def cis(phase, length, sign):
    ang = (np.asarray(phase, np.int64) % length).astype(np.float64) * (2 * np.pi / length)
    return np.cos(ang), sign * np.sin(ang)

def halves(mat):
    hi = mat.astype(np.float32).astype(bf16)
    lo = (mat - hi.astype(np.float64)).astype(np.float32).astype(bf16)
    return hi, lo

def tables():
    lane = np.arange(128)
    c, s = cis(np.outer(lane, lane), 128, -1)
    fwd = np.block([[c, s], [-s, c]])
    inv = np.block([[c, -s], [s, c]]) / N
    mats = np.stack([*halves(fwd), *halves(inv)])
    tile = np.arange(256)
    tw = np.stack(cis(np.outer(tile, lane), N, -1)).astype(np.float32)
    ij = np.outer(np.arange(16), np.arange(16)).reshape(256, 1) * np.ones((1, 128), np.int64)
    ct = np.stack(cis(ij, 256, -1)).astype(np.float32)
    return mats, np.concatenate([tw, ct])

R2 = math.sqrt(0.5)
C1, S1 = math.cos(math.pi / 8), math.sin(math.pi / 8)

def cadd(a, b): return (a[0] + b[0], a[1] + b[1])
def csub(a, b): return (a[0] - b[0], a[1] - b[1])

def turn16(a, p, sign):
    p = (sign * p) % 16
    q, r = divmod(p, 4)
    x, y = a
    if r == 2:
        x, y = ((x - y) * R2, (x + y) * R2)
    elif r:
        c, s = (C1, S1) if r == 1 else (S1, C1)
        x, y = (x * c - y * s, x * s + y * c)
    return [(x, y), (-y, x), (-x, -y), (y, -x)][q]

def fold4(a, b, c, d, sign):
    e, f, g, h = cadd(a, c), csub(a, c), cadd(b, d), csub(b, d)
    if sign > 0:
        t, u = (f[0] - h[1], f[1] + h[0]), (f[0] + h[1], f[1] - h[0])
    else:
        t, u = (f[0] + h[1], f[1] - h[0]), (f[0] - h[1], f[1] + h[0])
    return cadd(e, g), t, csub(e, g), u

def dft16(v, sign):
    cols = [fold4(v[b], v[b + 4], v[b + 8], v[b + 12], sign) for b in range(4)]
    out = [None] * 16
    for a in range(4):
        o = fold4(*[turn16(cols[b][a], a * b, sign) for b in range(4)], sign)
        for c in range(4):
            out[a + 4 * c] = o[c]
    return out

def dft8(v, sign):
    even = fold4(v[0], v[2], v[4], v[6], sign)
    odd = fold4(v[1], v[3], v[5], v[7], sign)
    odd = [turn16(o, 2 * i, sign) for i, o in enumerate(odd)]
    return [cadd(e, o) for e, o in zip(even, odd)] + [csub(e, o) for e, o in zip(even, odd)]

def half16(v, sign, flip):
    even = dft8(v[0::2], sign)
    odd = dft8([(flip * a, flip * b) for a, b in v[1::2]], sign)
    return [cadd(e, turn16(o, i, sign)) for i, (e, o) in enumerate(zip(even, odd))]

def cmul(a, c, s): return (a[0] * c - a[1] * s, a[0] * s + a[1] * c)
def cmulc(a, c, s): return (a[0] * c + a[1] * s, a[1] * c - a[0] * s)

def split(x):
    hi = x.astype(bf16)
    return hi, (x - hi.astype(f32)).astype(bf16)

def stage_j(xs, y, tab):
    def body(m1, _):
        lanes = pl.ds(pl.multiple_of(m1 * 128, 128), 128)
        v = [(xs[j, 0, :, lanes].astype(f32), xs[j, 1, :, lanes].astype(f32)) for j in range(16)]
        for k0, a in enumerate(dft16(v, -1)):
            if k0:
                row = pl.ds(m1 * 16 + k0, 1)
                a = cmul(a, tab[2, row, :], tab[3, row, :])
            y[0, k0 * 16 + m1], y[1, k0 * 16 + m1] = a
        return 0
    lax.fori_loop(0, 16, body, 0)

def put_pair(hi_ref, lo_ref, row, a, b):
    rows = pl.ds(pl.multiple_of(row, 16), 16)
    for part, lanes in ((0, slice(0, 128)), (1, slice(128, 256))):
        hi, lo = split(jnp.concatenate([a[part], b[part]], axis=0))
        hi_ref[rows, lanes] = hi
        lo_ref[rows, lanes] = lo

def stage_m(y, hi_ref, lo_ref, tab):
    def body(k0, _):
        out = dft16([(y[0, k0 * 16 + m1], y[1, k0 * 16 + m1]) for m1 in range(16)], -1)
        out = [cmul(a, tab[0, pl.ds(k0 + 16 * k1, 1), :], tab[1, pl.ds(k0 + 16 * k1, 1), :]) for k1, a in enumerate(out)]
        for k1 in range(0, 16, 2):
            put_pair(hi_ref, lo_ref, k0 * 128 + k1 * 8, out[k1], out[k1 + 1])
        return 0
    lax.fori_loop(0, 16, body, 0)

def dot3(hi, lo, whi, wlo):
    d = functools.partial(jnp.dot, preferred_element_type=f32)
    return d(hi, whi) + d(lo, whi) + d(hi, wlo)

def ahead(hi_ref, lo_ref, q, mats, chunk=512):
    def body(i, _):
        rows = pl.ds(pl.multiple_of(i * chunk, chunk), chunk)
        q[rows, :] = dot3(hi_ref[rows, :], lo_ref[rows, :], mats[0], mats[1])
        return 0
    lax.fori_loop(0, 2048 // chunk, body, 0)

def weigh(q, hi_ref, lo_ref, resp, chunk=128):
    def body(i, _):
        rows = pl.ds(pl.multiple_of(i * chunk, chunk), chunk)
        p = cmul((q[rows, 0:128], q[rows, 128:256]), resp[0, rows, :], resp[1, rows, :])
        for part, lanes in ((0, slice(0, 128)), (1, slice(128, 256))):
            hi, lo = split(p[part])
            hi_ref[rows, lanes] = hi
            lo_ref[rows, lanes] = lo
        return 0
    lax.fori_loop(0, 2048 // chunk, body, 0)

def mid(hi_ref, lo_ref, resp, mats, chunk=512):
    def body(i, _):
        rows = pl.ds(pl.multiple_of(i * chunk, chunk), chunk)
        s = dot3(hi_ref[rows, :], lo_ref[rows, :], mats[0], mats[1])
        p = cmul((s[:, :128], s[:, 128:]), resp[0, rows, :], resp[1, rows, :])
        for part, lanes in ((0, slice(0, 128)), (1, slice(128, 256))):
            hi, lo = split(p[part])
            hi_ref[rows, lanes] = hi
            lo_ref[rows, lanes] = lo
        return 0
    lax.fori_loop(0, 2048 // chunk, body, 0)

def back(hi_ref, lo_ref, q, mats, chunk=512):
    def body(i, _):
        rows = pl.ds(pl.multiple_of(i * chunk, chunk), chunk)
        q[rows, :] = dot3(hi_ref[rows, :], lo_ref[rows, :], mats[2], mats[3])
        return 0
    lax.fori_loop(0, 2048 // chunk, body, 0)

def stage_k1(q, y, tab):
    def body(k0, _):
        v = []
        for k1 in range(16):
            rows = pl.ds(pl.multiple_of(k0 * 128 + k1 * 8, 8), 8)
            row = pl.ds(k0 + 16 * k1, 1)
            v.append(cmulc((q[rows, 0:128], q[rows, 128:256]), tab[0, row, :], tab[1, row, :]))
        for m1, a in enumerate(dft16(v, 1)):
            y[0, k0 * 16 + m1], y[1, k0 * 16 + m1] = a
        return 0
    lax.fori_loop(0, 16, body, 0)

def stage_k0(y, out, tab, flip, g):
    def body(m1, _):
        v = []
        for k0 in range(16):
            a = (y[0, k0 * 16 + m1], y[1, k0 * 16 + m1])
            if k0:
                row = pl.ds(m1 * 16 + k0, 1)
                a = cmulc(a, tab[2, row, :], tab[3, row, :])
            v.append(a)
        for j, a in enumerate(half16(v, 1, flip)):
            lanes = pl.ds(pl.multiple_of(j * 2048 + m1 * 128, 128), 128)
            out[0, 8 * g:8 * g + 8, lanes], out[1, 8 * g:8 * g + 8, lanes] = a
        return 0
    lax.fori_loop(0, 16, body, 0)

def phase(idx):
    idx = (idx & (N - 1))
    idx = jnp.where(idx >= N // 2, idx - N, idx)
    ang = idx.astype(f32) * (2 * math.pi / N)
    return jnp.cos(ang), -jnp.sin(ang)

def response(bank, slabs, shifts, resp, groups):
    sub = lax.broadcasted_iota(jnp.int32, (8, 128), 0)
    lane = lax.broadcasted_iota(jnp.int32, (8, 128), 1)
    for g in groups:
        def body(r, _):
            sl = slabs[8 * g + r]
            sh = shifts[8 * g + r]
            e = [phase((16 * (sub + 8 * h) + 256 * lane) * sh) for h in range(2)]
            w = phase(jnp.full((8, 128), 1, jnp.int32) * sh)
            for i in range(16):
                hr = bank[0, sl, 16 * i:16 * i + 16, :].astype(f32)
                hi = bank[1, sl, 16 * i:16 * i + 16, :].astype(f32)
                for h in range(2):
                    o = cmul((hr[8 * h:8 * h + 8], hi[8 * h:8 * h + 8]), *e[h])
                    rows = pl.ds((16 * i + 8 * h) * 8 + r, 8, stride=8)
                    resp[g, 0, rows, :] = o[0]
                    resp[g, 1, rows, :] = o[1]
                if i < 15:
                    e = [cmul(x, *w) for x in e]
            return 0
        lax.fori_loop(0, 8, body, 0)


def place_filters(raw, lines, turned, bank, part, chunk):
    def spread(i, _):
        lanes = pl.ds(pl.multiple_of(i * 2048, 2048), 2048)
        block = raw[:, lanes].astype(f32)
        for t in range(16):
            for slab in range(2):
                lines[slab, pl.ds(i * 16 + t, 1), :] = block[slab:slab + 1, 128 * t:128 * t + 128]
        return 0
    lax.fori_loop(0, 16, spread, 0)
    for slab in range(2):
        for h in range(2):
            flat = jnp.transpose(lines[slab, pl.ds(h, 128, stride=2), :])
            for b in range(8):
                turned[slab, pl.ds(8 * h + b, 16, stride=16), :] = flat[16 * b:16 * b + 16]
        bank[part, 2 * chunk + slab] = turned[slab].astype(bf16)


def kernel(
    echoes, filters, slabs, shifts, mats_h, tab_h, out,
    xs, est, bank, raw, lines, turned, mats, tab, y, ahi, alo, q, resp,
    loc, es, er, fs, fr, zs, zr, cs, cr,
):
    t, b, s = (lax.axis_index(n) for n in ("turn", "blk", "strip"))
    yy, core = t // 2, t % 2
    xlo, z = b // 8, b % 8
    xx = 2 * s + xlo

    def at_y(dy, dc):
        return (((yy + dy) % 4) * 2 + (core + dc) % 2, b, s)

    def at_x(d):
        x = (xx + d) % 4
        return (t, (x % 2) * 8 + z, x // 2)

    def at_z(d):
        return (t, xlo * 8 + (z + d) % 8, s)

    mate, twin = at_y(0, 1), (t, b, 1 - s)
    peers = [at_y(dy, dc) for dy, dc in ((0, 1), (1, 0), (3, 0), (1, 1), (3, 1), (2, 0), (2, 1))]

    barrier = pltpu.get_barrier_semaphore()
    known = peers + [twin, at_x(1), at_x(3), at_z(1), at_z(7)]
    for d in known:
        pl.semaphore_signal(barrier, inc=1, device_id=d, device_id_type=MESH)

    mine = 2 * t + s
    local = [
        pltpu.make_async_copy(filters.at[core], raw, loc.at[0]),
        pltpu.make_async_copy(echoes, est, loc.at[1]),
        pltpu.make_async_copy(echoes.at[:, t, 0], xs.at[0, mine], loc.at[2]),
        pltpu.make_async_copy(echoes.at[:, t, 1], xs.at[1, mine], loc.at[3]),
        pltpu.make_async_copy(mats_h, mats, loc.at[4]),
        pltpu.make_async_copy(tab_h, tab, loc.at[5]),
    ]
    for c in local:
        c.start()
    local[0].wait()
    place_filters(raw, lines, turned, bank, core, b)
    for c in local[1:]:
        c.wait()
    pl.semaphore_wait(barrier, len(known))

    sent = []

    def send(src, dst, ssem, rsem, device):
        c = pltpu.make_async_remote_copy(
            src, dst, ssem, rsem, device_id=device, device_id_type=MESH
        )
        c.start()
        sent.append(c)

    def arrived(ref, ssem, rsem):
        pltpu.make_async_remote_copy(
            ref, ref, ssem, rsem, device_id=twin, device_id_type=MESH
        ).wait_recv()

    def slot(device):
        return 2 * device[0] + s

    def forward(g, j):
        ref = xs.at[g, j]
        send(ref, ref, es.at[g, j], er.at[g, j], twin)

    def echo(g, device):
        j = slot(device)
        arrived(xs.at[g, j], es.at[g, j], er.at[g, j])
        forward(g, j)

    def slab(part, n, d):
        side = xlo if n < 2 else 1 - xlo
        return bank.at[part, 2 * (side * 8 + (z + d) % 8) + n % 2]

    def over_z(n, hop, way):
        ref = slab(core, n, (1 - hop if way == 0 else hop - 1) % 8)
        send(ref, ref, zs.at[way, hop - 1, n], zr.at[way, hop - 1, n], at_z(1 if way == 0 else 7))

    def over_core(n, d):
        ref = slab(core, n, d)
        send(ref, ref, cs.at[n, d], cr.at[n, d], mate)

    def relay(u, hop):
        for i in range(2):
            n = 2 * u + i
            for way in range(2):
                if hop == 4 and way != i:
                    continue
                d = (-hop if way == 0 else hop) % 8
                arrived(slab(core, n, d), zs.at[way, hop - 1, n], zr.at[way, hop - 1, n])
                if hop < 3 or (hop == 3 and way == i):
                    over_z(n, hop + 1, way)
                over_core(n, d)

    def own_filters():
        for i, d in ((0, 1), (1, 3)):
            ref = slab(core, i, 0)
            send(ref, ref, fs.at[i], fr.at[i], at_x(d))
        for i in range(2):
            over_z(i, 1, 0)
            over_z(i, 1, 1)

    def other_filters():
        for i in range(2):
            arrived(slab(core, 2 + i, 0), fs.at[i], fr.at[i])
            over_z(2 + i, 1, 0)
            over_z(2 + i, 1, 1)
            over_core(2 + i, 0)

    def over_y(g):
        for k, d in enumerate(peers):
            send(est.at[:, d[0], g], xs.at[g, mine], loc.at[8 + 8 * g + k], er.at[g, mine], d)

    def echoes_in(g):
        for k in range(8):
            j = 2 * k + 1 - s
            arrived(xs.at[g, j], es.at[g, j], er.at[g, j])

    def filters_in():
        for n in range(4):
            for d in range(8):
                arrived(slab(1 - core, n, d), cs.at[n, d], cr.at[n, d])

    flip = 1.0 - 2.0 * s.astype(f32)

    own_filters()
    forward(0, mine)
    over_y(0)
    for i in range(2): over_core(i, 0)
    echo(0, peers[0])
    other_filters()
    for d in peers[1:3]: echo(0, d)
    relay(0, 1)
    for d in peers[3:5]: echo(0, d)
    relay(1, 1)
    forward(1, mine)
    over_y(1)
    for d in peers[5:]: echo(0, d)
    echo(1, peers[0])
    relay(0, 2)
    for d in peers[1:3]: echo(1, d)
    relay(1, 2)
    for d in peers[3:5]: echo(1, d)
    for d in peers[5:]: echo(1, d)
    relay(0, 3)
    echoes_in(0)
    stage_j(xs.at[0], y, tab)
    relay(1, 3)
    stage_m(y, ahi, alo, tab)
    relay(0, 4)
    ahead(ahi, alo, q, mats)
    relay(1, 4)
    filters_in()
    response(bank, slabs, shifts, resp, (0, 1))
    weigh(q, ahi, alo, resp.at[0])
    back(ahi, alo, q, mats)
    stage_k1(q, y, tab)
    stage_k0(y, out, tab, flip, 0)
    echoes_in(1)
    stage_j(xs.at[1], y, tab)
    stage_m(y, ahi, alo, tab)
    ahead(ahi, alo, q, mats)
    weigh(q, ahi, alo, resp.at[1])
    back(ahi, alo, q, mats)
    stage_k1(q, y, tab)
    stage_k0(y, out, tab, flip, 1)
    for c in sent:
        c.wait_send()


def per_device(echoes, filters, slab_index, shifts):
    mats, tab = tables()
    hbm = pl.BlockSpec(memory_space=pl.ANY)
    smem = pl.BlockSpec(memory_space=pltpu.SMEM)
    dma = pltpu.SemaphoreType.DMA
    return pl.pallas_call(
        kernel,
        out_shape=pltpu.VMEM((2, 16, N // 2), f32),
        in_specs=[hbm, hbm, smem, smem, hbm, hbm],
        out_specs=pl.BlockSpec(memory_space=pltpu.VMEM),
        scratch_shapes=[
            pltpu.VMEM((2, 16, 2, 8, 2048), bf16),
            pltpu.VMEM((2, 8, 2, 8, 2048), bf16),
            pltpu.VMEM((2, 32, 256, 128), bf16),
            pltpu.VMEM((2, N), bf16),
            pltpu.VMEM((2, 256, 128), f32),
            pltpu.VMEM((2, 256, 128), f32),
            pltpu.VMEM((4, 256, 256), bf16),
            pltpu.VMEM((4, 256, 128), f32),
            pltpu.VMEM((2, 256, 8, 128), f32),
            pltpu.VMEM((2048, 256), bf16),
            pltpu.VMEM((2048, 256), bf16),
            pltpu.VMEM((2048, 256), f32),
            pltpu.VMEM((2, 2, 2048, 128), f32),
            dma((24,)),
            dma((2, 16)),
            dma((2, 16)),
            dma((2,)),
            dma((2,)),
            dma((2, 4, 4)),
            dma((2, 4, 4)),
            dma((4, 8)),
            dma((4, 8)),
        ],
        compiler_params=pltpu.CompilerParams(
            collective_id=0, has_side_effects=True, vmem_limit_bytes=64946176
        ),
    )(
        echoes.reshape(2, 8, 2, 8, 2048), filters, slab_index, shifts,
        jnp.asarray(mats), jnp.asarray(tab),
    )


def solution(mesh):
    in_specs = (
        P(None, "blk", ("turn", "strip")),
        P(None, "blk", None),
        P(("blk", "turn")),
        P(("blk", "turn")),
    )
    out_specs = P(None, ("blk", "turn"), "strip")
    return jax.shard_map(
        per_device, mesh=mesh, in_specs=in_specs, out_specs=out_specs, check_vma=False
    )
```

```python
import functools
import math

import numpy as np
import jax
import jax.numpy as jnp
from jax import lax
from jax.experimental import pallas as pl
from jax.experimental.pallas import tpu as pltpu
from jax.sharding import PartitionSpec as P

N = 32768
f32, bf16 = jnp.float32, jnp.bfloat16
MESH = pl.DeviceIdType.MESH

def cis(phase, length, sign):
    ang = (np.asarray(phase, np.int64) % length).astype(np.float64) * (2 * np.pi / length)
    return np.cos(ang), sign * np.sin(ang)

def halves(mat):
    hi = mat.astype(np.float32).astype(bf16)
    lo = (mat - hi.astype(np.float64)).astype(np.float32).astype(bf16)
    return hi, lo

def tables():
    lane = np.arange(128)
    c, s = cis(np.outer(lane, lane), 128, -1)
    fwd = np.block([[c, s], [-s, c]])
    inv = np.block([[c, -s], [s, c]]) / N
    mats = np.stack([*halves(fwd), *halves(inv)])
    tile = np.arange(256)
    tw = np.stack(cis(np.outer(tile, lane), N, -1)).astype(np.float32)
    ij = np.outer(np.arange(16), np.arange(16)).reshape(256, 1) * np.ones((1, 128), np.int64)
    ct = np.stack(cis(ij, 256, -1)).astype(np.float32)
    return mats, np.concatenate([tw, ct])

R2 = math.sqrt(0.5)
C1, S1 = math.cos(math.pi / 8), math.sin(math.pi / 8)

def cadd(a, b): return (a[0] + b[0], a[1] + b[1])
def csub(a, b): return (a[0] - b[0], a[1] - b[1])

def turn16(a, p, sign):
    p = (sign * p) % 16
    q, r = divmod(p, 4)
    x, y = a
    if r == 2:
        x, y = ((x - y) * R2, (x + y) * R2)
    elif r:
        c, s = (C1, S1) if r == 1 else (S1, C1)
        x, y = (x * c - y * s, x * s + y * c)
    return [(x, y), (-y, x), (-x, -y), (y, -x)][q]

def fold4(a, b, c, d, sign):
    e, f, g, h = cadd(a, c), csub(a, c), cadd(b, d), csub(b, d)
    if sign > 0:
        t, u = (f[0] - h[1], f[1] + h[0]), (f[0] + h[1], f[1] - h[0])
    else:
        t, u = (f[0] + h[1], f[1] - h[0]), (f[0] - h[1], f[1] + h[0])
    return cadd(e, g), t, csub(e, g), u

def dft16(v, sign):
    cols = [fold4(v[b], v[b + 4], v[b + 8], v[b + 12], sign) for b in range(4)]
    out = [None] * 16
    for a in range(4):
        o = fold4(*[turn16(cols[b][a], a * b, sign) for b in range(4)], sign)
        for c in range(4):
            out[a + 4 * c] = o[c]
    return out

def dft8(v, sign):
    even = fold4(v[0], v[2], v[4], v[6], sign)
    odd = fold4(v[1], v[3], v[5], v[7], sign)
    odd = [turn16(o, 2 * i, sign) for i, o in enumerate(odd)]
    return [cadd(e, o) for e, o in zip(even, odd)] + [csub(e, o) for e, o in zip(even, odd)]

def half16(v, sign, flip):
    even = dft8(v[0::2], sign)
    odd = dft8([(flip * a, flip * b) for a, b in v[1::2]], sign)
    return [cadd(e, turn16(o, i, sign)) for i, (e, o) in enumerate(zip(even, odd))]

def cmul(a, c, s): return (a[0] * c - a[1] * s, a[0] * s + a[1] * c)
def cmulc(a, c, s): return (a[0] * c + a[1] * s, a[1] * c - a[0] * s)

def split(x):
    hi = x.astype(bf16)
    return hi, (x - hi.astype(f32)).astype(bf16)

def stage_j(xs, y, tab):
    def body(m1, _):
        lanes = pl.ds(pl.multiple_of(m1 * 128, 128), 128)
        v = [(xs[j, 0, :, lanes].astype(f32), xs[j, 1, :, lanes].astype(f32)) for j in range(16)]
        for k0, a in enumerate(dft16(v, -1)):
            if k0:
                row = pl.ds(m1 * 16 + k0, 1)
                a = cmul(a, tab[2, row, :], tab[3, row, :])
            y[0, k0 * 16 + m1], y[1, k0 * 16 + m1] = a
        return 0
    lax.fori_loop(0, 16, body, 0)

def put_pair(hi_ref, lo_ref, row, a, b):
    rows = pl.ds(pl.multiple_of(row, 16), 16)
    for part, lanes in ((0, slice(0, 128)), (1, slice(128, 256))):
        hi, lo = split(jnp.concatenate([a[part], b[part]], axis=0))
        hi_ref[rows, lanes] = hi
        lo_ref[rows, lanes] = lo

def stage_m(y, hi_ref, lo_ref, tab):
    def body(k0, _):
        out = dft16([(y[0, k0 * 16 + m1], y[1, k0 * 16 + m1]) for m1 in range(16)], -1)
        out = [cmul(a, tab[0, pl.ds(k0 + 16 * k1, 1), :], tab[1, pl.ds(k0 + 16 * k1, 1), :]) for k1, a in enumerate(out)]
        for k1 in range(0, 16, 2):
            put_pair(hi_ref, lo_ref, k0 * 128 + k1 * 8, out[k1], out[k1 + 1])
        return 0
    lax.fori_loop(0, 16, body, 0)

def dot3(hi, lo, whi, wlo):
    d = functools.partial(jnp.dot, preferred_element_type=f32)
    return d(hi, whi) + d(lo, whi) + d(hi, wlo)

def ahead_part(i, hi_ref, lo_ref, q, mats, chunk):
    rows = pl.ds(pl.multiple_of(i * chunk, chunk), chunk)
    q[rows, :] = dot3(hi_ref[rows, :], lo_ref[rows, :], mats[0], mats[1])

def ahead(hi_ref, lo_ref, q, mats, chunk=1024):
    def body(i, _):
        ahead_part(i, hi_ref, lo_ref, q, mats, chunk)
        return 0
    lax.fori_loop(0, 2048 // chunk, body, 0)

def weigh_back(i, q, resp, mats, chunk):
    rows = pl.ds(pl.multiple_of(i * chunk, chunk), chunk)
    p = cmul((q[rows, 0:128], q[rows, 128:256]), resp[0, rows, :], resp[1, rows, :])
    hi, lo = split(jnp.concatenate(p, axis=1))
    q[rows, :] = dot3(hi, lo, mats[2], mats[3])

def stage_k1(k0, q, y, tab):
    v = []
    for k1 in range(16):
        rows = pl.ds(pl.multiple_of(k0 * 128 + k1 * 8, 8), 8)
        row = pl.ds(k0 + 16 * k1, 1)
        v.append(cmulc((q[rows, 0:128], q[rows, 128:256]), tab[0, row, :], tab[1, row, :]))
    for m1, a in enumerate(dft16(v, 1)):
        y[0, k0 * 16 + m1], y[1, k0 * 16 + m1] = a

def stage_k0(y, out, tab, flip, g):
    def body(m1, _):
        v = []
        for k0 in range(16):
            a = (y[0, k0 * 16 + m1], y[1, k0 * 16 + m1])
            if k0:
                row = pl.ds(m1 * 16 + k0, 1)
                a = cmulc(a, tab[2, row, :], tab[3, row, :])
            v.append(a)
        for j, a in enumerate(half16(v, 1, flip)):
            lanes = pl.ds(pl.multiple_of(j * 2048 + m1 * 128, 128), 128)
            rows = pl.ds(pl.multiple_of(8 * g, 8), 8)
            out[0, rows, lanes], out[1, rows, lanes] = a
        return 0
    lax.fori_loop(0, 16, body, 0)

def phase(idx):
    idx = (idx & (N - 1))
    idx = jnp.where(idx >= N // 2, idx - N, idx)
    ang = idx.astype(f32) * (2 * math.pi / N)
    return jnp.cos(ang), -jnp.sin(ang)

def response(line, r, bank, slabs, shifts, resp):
    sub = lax.broadcasted_iota(jnp.int32, (8, 128), 0)
    lane = lax.broadcasted_iota(jnp.int32, (8, 128), 1)
    sl, sh = slabs[line], shifts[line]
    e = [phase((16 * (sub + 8 * h) + 256 * lane) * sh) for h in range(2)]
    w = phase(jnp.full((8, 128), 1, jnp.int32) * sh)
    for i in range(16):
        hr = bank[0, sl, 16 * i:16 * i + 16, :].astype(f32)
        hi = bank[1, sl, 16 * i:16 * i + 16, :].astype(f32)
        for h in range(2):
            o = cmul((hr[8 * h:8 * h + 8], hi[8 * h:8 * h + 8]), *e[h])
            rows = pl.ds((16 * i + 8 * h) * 8 + r, 8, stride=8)
            resp[0, rows, :] = o[0]
            resp[1, rows, :] = o[1]
        if i < 15:
            e = [cmul(x, *w) for x in e]


def place_filters(raw, lines, turned, bank, part, chunk):
    def spread(i, _):
        lanes = pl.ds(pl.multiple_of(i * 2048, 2048), 2048)
        block = raw[:, lanes].astype(f32)
        for t in range(16):
            for slab in range(2):
                lines[slab, pl.ds(i * 16 + t, 1), :] = block[slab:slab + 1, 128 * t:128 * t + 128]
        return 0
    lax.fori_loop(0, 16, spread, 0)
    for slab in range(2):
        for h in range(2):
            flat = jnp.transpose(lines[slab, pl.ds(h, 128, stride=2), :])
            for b in range(8):
                turned[slab, pl.ds(8 * h + b, 16, stride=16), :] = flat[16 * b:16 * b + 16]
        bank[part, 2 * chunk + slab] = turned[slab].astype(bf16)


def kernel(
    echoes, filters, slabs, shifts, mats_h, tab_h, out,
    xs, est, bank, raw, lines, turned, mats, tab, y, ahi, alo, q0, q1, resp0, resp1,
    loc, es, er, fs, fr, zs, zr, cs, cr,
):
    t, b, s = (lax.axis_index(n) for n in ("turn", "blk", "strip"))
    yy, core = t // 2, t % 2
    xlo, z = b // 8, b % 8
    xx = 2 * s + xlo

    def at_y(dy, dc):
        return (((yy + dy) % 4) * 2 + (core + dc) % 2, b, s)

    def at_x(d):
        x = (xx + d) % 4
        return (t, (x % 2) * 8 + z, x // 2)

    def at_z(d):
        return (t, xlo * 8 + (z + d) % 8, s)

    mate, twin = at_y(0, 1), (t, b, 1 - s)
    peers = [at_y(dy, dc) for dy, dc in ((0, 1), (1, 0), (3, 0), (1, 1), (3, 1), (2, 0), (2, 1))]

    barrier = pltpu.get_barrier_semaphore()
    known = peers + [twin, at_x(1), at_x(3), at_z(1), at_z(7)]
    for d in known:
        pl.semaphore_signal(barrier, inc=1, device_id=d, device_id_type=MESH)

    mine = 2 * t + s
    local = [
        pltpu.make_async_copy(filters.at[core], raw, loc.at[0]),
        pltpu.make_async_copy(echoes, est, loc.at[1]),
        pltpu.make_async_copy(echoes.at[:, t, 0], xs.at[0, mine], loc.at[2]),
        pltpu.make_async_copy(echoes.at[:, t, 1], xs.at[1, mine], loc.at[3]),
        pltpu.make_async_copy(mats_h, mats, loc.at[4]),
        pltpu.make_async_copy(tab_h, tab, loc.at[5]),
    ]
    for c in local:
        c.start()
    local[0].wait()
    place_filters(raw, lines, turned, bank, core, b)
    for c in local[1:]:
        c.wait()
    pl.semaphore_wait(barrier, len(known))

    sent = []

    def send(src, dst, ssem, rsem, device):
        c = pltpu.make_async_remote_copy(
            src, dst, ssem, rsem, device_id=device, device_id_type=MESH
        )
        c.start()
        sent.append(c)

    def arrived(ref, ssem, rsem):
        pltpu.make_async_remote_copy(
            ref, ref, ssem, rsem, device_id=twin, device_id_type=MESH
        ).wait_recv()

    def slot(device):
        return 2 * device[0] + s

    def forward(g, j):
        ref = xs.at[g, j]
        send(ref, ref, es.at[g, j], er.at[g, j], twin)

    def echo(g, device):
        j = slot(device)
        arrived(xs.at[g, j], es.at[g, j], er.at[g, j])
        forward(g, j)

    def slab(part, n, d):
        side = xlo if n < 2 else 1 - xlo
        return bank.at[part, 2 * (side * 8 + (z + d) % 8) + n % 2]

    def over_z(n, hop, way):
        ref = slab(core, n, (1 - hop if way == 0 else hop - 1) % 8)
        send(ref, ref, zs.at[way, hop - 1, n], zr.at[way, hop - 1, n], at_z(1 if way == 0 else 7))

    def over_core(n, d):
        ref = slab(core, n, d)
        send(ref, ref, cs.at[n, d], cr.at[n, d], mate)

    def relay(u, hop):
        for i in range(2):
            n = 2 * u + i
            for way in range(2):
                if hop == 4 and way != i:
                    continue
                d = (-hop if way == 0 else hop) % 8
                arrived(slab(core, n, d), zs.at[way, hop - 1, n], zr.at[way, hop - 1, n])
                if hop < 3 or (hop == 3 and way == i):
                    over_z(n, hop + 1, way)
                over_core(n, d)

    def own_filters():
        for i, d in ((0, 1), (1, 3)):
            ref = slab(core, i, 0)
            send(ref, ref, fs.at[i], fr.at[i], at_x(d))
        for i in range(2):
            over_z(i, 1, 0)
            over_z(i, 1, 1)

    def other_filters():
        for i in range(2):
            arrived(slab(core, 2 + i, 0), fs.at[i], fr.at[i])
            over_z(2 + i, 1, 0)
            over_z(2 + i, 1, 1)
            over_core(2 + i, 0)

    def over_y(g):
        for k, d in enumerate(peers):
            send(est.at[:, d[0], g], xs.at[g, mine], loc.at[8 + 8 * g + k], er.at[g, mine], d)

    def echoes_in(g):
        for k in range(8):
            j = 2 * k + 1 - s
            arrived(xs.at[g, j], es.at[g, j], er.at[g, j])

    def filters_in():
        for n in range(4):
            for d in range(8):
                arrived(slab(1 - core, n, d), cs.at[n, d], cr.at[n, d])

    flip = 1.0 - 2.0 * s.astype(f32)

    own_filters()
    forward(0, mine)
    over_y(0)
    for i in range(2): over_core(i, 0)
    echo(0, peers[0])
    other_filters()
    for d in peers[1:3]: echo(0, d)
    relay(0, 1)
    for d in peers[3:5]: echo(0, d)
    relay(1, 1)
    forward(1, mine)
    over_y(1)
    for d in peers[5:]: echo(0, d)
    echo(1, peers[0])
    relay(0, 2)
    for d in peers[1:3]: echo(1, d)
    relay(1, 2)
    for d in peers[3:5]: echo(1, d)
    for d in peers[5:]: echo(1, d)
    relay(0, 3)

    echoes_in(0)
    stage_j(xs.at[0], y, tab)
    relay(1, 3)
    stage_m(y, ahi, alo, tab)
    relay(0, 4)
    ahead(ahi, alo, q0, mats)
    relay(1, 4)

    echoes_in(1)
    stage_j(xs.at[1], y, tab)
    stage_m(y, ahi, alo, tab)
    filters_in()

    def shape(i, _):
        ahead_part(i, ahi, alo, q1, mats, 512)
        for half in range(2):
            response(2 * i + half, 2 * i + half, bank, slabs, shifts, resp0)
            response(8 + 2 * i + half, 2 * i + half, bank, slabs, shifts, resp1)
        return 0

    lax.fori_loop(0, 4, shape, 0)

    def first(i, _):
        weigh_back(i, q0, resp0, mats, 512)
        return 0

    lax.fori_loop(0, 4, first, 0)

    def second(i, _):
        weigh_back(i, q1, resp1, mats, 512)
        for n in range(4):
            stage_k1(4 * i + n, q0, y, tab)
        return 0

    lax.fori_loop(0, 4, second, 0)
    stage_k0(y, out, tab, flip, 0)

    def last(k0, _):
        stage_k1(k0, q1, y, tab)
        return 0

    lax.fori_loop(0, 16, last, 0)
    stage_k0(y, out, tab, flip, 1)
    for c in sent:
        c.wait_send()


def per_device(echoes, filters, slab_index, shifts):
    mats, tab = tables()
    hbm = pl.BlockSpec(memory_space=pl.ANY)
    smem = pl.BlockSpec(memory_space=pltpu.SMEM)
    dma = pltpu.SemaphoreType.DMA
    return pl.pallas_call(
        kernel,
        out_shape=pltpu.VMEM((2, 16, N // 2), f32),
        in_specs=[hbm, hbm, smem, smem, hbm, hbm],
        out_specs=pl.BlockSpec(memory_space=pltpu.VMEM),
        scratch_shapes=[
            pltpu.VMEM((2, 16, 2, 8, 2048), bf16),
            pltpu.VMEM((2, 8, 2, 8, 2048), bf16),
            pltpu.VMEM((2, 32, 256, 128), bf16),
            pltpu.VMEM((2, N), bf16),
            pltpu.VMEM((2, 256, 128), f32),
            pltpu.VMEM((2, 256, 128), f32),
            pltpu.VMEM((4, 256, 256), bf16),
            pltpu.VMEM((4, 256, 128), f32),
            pltpu.VMEM((2, 256, 8, 128), f32),
            pltpu.VMEM((2048, 256), bf16),
            pltpu.VMEM((2048, 256), bf16),
            pltpu.VMEM((2048, 256), f32),
            pltpu.VMEM((2048, 256), f32),
            pltpu.VMEM((2, 2048, 128), f32),
            pltpu.VMEM((2, 2048, 128), f32),
            dma((24,)),
            dma((2, 16)),
            dma((2, 16)),
            dma((2,)),
            dma((2,)),
            dma((2, 4, 4)),
            dma((2, 4, 4)),
            dma((4, 8)),
            dma((4, 8)),
        ],
        compiler_params=pltpu.CompilerParams(
            collective_id=0, has_side_effects=True, vmem_limit_bytes=64946176
        ),
    )(
        echoes.reshape(2, 8, 2, 8, 2048), filters, slab_index, shifts,
        jnp.asarray(mats), jnp.asarray(tab),
    )


def solution(mesh):
    in_specs = (
        P(None, "blk", ("turn", "strip")),
        P(None, "blk", None),
        P(("blk", "turn")),
        P(("blk", "turn")),
    )
    out_specs = P(None, ("blk", "turn"), "strip")
    return jax.shard_map(
        per_device, mesh=mesh, in_specs=in_specs, out_specs=out_specs, check_vma=False
    )
```

```python
import functools
import math

import numpy as np
import jax
import jax.numpy as jnp
from jax import lax
from jax.experimental import pallas as pl
from jax.experimental.pallas import tpu as pltpu
from jax.sharding import PartitionSpec as P

N = 32768
f32, bf16 = jnp.float32, jnp.bfloat16
MESH = pl.DeviceIdType.MESH

def cis(phase, length, sign):
    ang = (np.asarray(phase, np.int64) % length).astype(np.float64) * (2 * np.pi / length)
    return np.cos(ang), sign * np.sin(ang)

def halves(mat):
    hi = mat.astype(np.float32).astype(bf16)
    lo = (mat - hi.astype(np.float64)).astype(np.float32).astype(bf16)
    return hi, lo

def tables():
    lane = np.arange(128)
    c, s = cis(np.outer(lane, lane), 128, -1)
    fwd = np.block([[c, s], [-s, c]])
    inv = np.block([[c, -s], [s, c]]) / N
    mats = np.stack([*halves(fwd), *halves(inv)])
    tile = np.arange(256)
    tw = np.stack(cis(np.outer(tile, lane), N, -1)).astype(np.float32)
    ij = np.outer(np.arange(16), np.arange(16)).reshape(256, 1) * np.ones((1, 128), np.int64)
    ct = np.stack(cis(ij, 256, -1)).astype(np.float32)
    return mats, np.concatenate([tw, ct])

R2 = math.sqrt(0.5)
C1, S1 = math.cos(math.pi / 8), math.sin(math.pi / 8)

def cadd(a, b): return (a[0] + b[0], a[1] + b[1])
def csub(a, b): return (a[0] - b[0], a[1] - b[1])

def turn16(a, p, sign):
    p = (sign * p) % 16
    q, r = divmod(p, 4)
    x, y = a
    if r == 2:
        x, y = ((x - y) * R2, (x + y) * R2)
    elif r:
        c, s = (C1, S1) if r == 1 else (S1, C1)
        x, y = (x * c - y * s, x * s + y * c)
    return [(x, y), (-y, x), (-x, -y), (y, -x)][q]

def fold4(a, b, c, d, sign):
    e, f, g, h = cadd(a, c), csub(a, c), cadd(b, d), csub(b, d)
    if sign > 0:
        t, u = (f[0] - h[1], f[1] + h[0]), (f[0] + h[1], f[1] - h[0])
    else:
        t, u = (f[0] + h[1], f[1] - h[0]), (f[0] - h[1], f[1] + h[0])
    return cadd(e, g), t, csub(e, g), u

def dft16(v, sign):
    cols = [fold4(v[b], v[b + 4], v[b + 8], v[b + 12], sign) for b in range(4)]
    out = [None] * 16
    for a in range(4):
        o = fold4(*[turn16(cols[b][a], a * b, sign) for b in range(4)], sign)
        for c in range(4):
            out[a + 4 * c] = o[c]
    return out

def dft8(v, sign):
    even = fold4(v[0], v[2], v[4], v[6], sign)
    odd = fold4(v[1], v[3], v[5], v[7], sign)
    odd = [turn16(o, 2 * i, sign) for i, o in enumerate(odd)]
    return [cadd(e, o) for e, o in zip(even, odd)] + [csub(e, o) for e, o in zip(even, odd)]

def half16(v, sign, flip):
    even = dft8(v[0::2], sign)
    odd = dft8([(flip * a, flip * b) for a, b in v[1::2]], sign)
    return [cadd(e, turn16(o, i, sign)) for i, (e, o) in enumerate(zip(even, odd))]

def cmul(a, c, s): return (a[0] * c - a[1] * s, a[0] * s + a[1] * c)
def cmulc(a, c, s): return (a[0] * c + a[1] * s, a[1] * c - a[0] * s)

def split(x):
    hi = x.astype(bf16)
    return hi, (x - hi.astype(f32)).astype(bf16)

def stage_j(xs, y, tab):
    def body(m1, _):
        lanes = pl.ds(pl.multiple_of(m1 * 128, 128), 128)
        v = [(xs[j, 0, :, lanes].astype(f32), xs[j, 1, :, lanes].astype(f32)) for j in range(16)]
        for k0, a in enumerate(dft16(v, -1)):
            if k0:
                row = pl.ds(m1 * 16 + k0, 1)
                a = cmul(a, tab[2, row, :], tab[3, row, :])
            y[0, k0 * 16 + m1], y[1, k0 * 16 + m1] = a
        return 0
    lax.fori_loop(0, 16, body, 0)

def put_pair(hi_ref, lo_ref, row, a, b):
    rows = pl.ds(pl.multiple_of(row, 16), 16)
    for part, lanes in ((0, slice(0, 128)), (1, slice(128, 256))):
        hi, lo = split(jnp.concatenate([a[part], b[part]], axis=0))
        hi_ref[rows, lanes] = hi
        lo_ref[rows, lanes] = lo

def stage_m(y, hi_ref, lo_ref, tab):
    def body(k0, _):
        out = dft16([(y[0, k0 * 16 + m1], y[1, k0 * 16 + m1]) for m1 in range(16)], -1)
        out = [cmul(a, tab[0, pl.ds(k0 + 16 * k1, 1), :], tab[1, pl.ds(k0 + 16 * k1, 1), :]) for k1, a in enumerate(out)]
        for k1 in range(0, 16, 2):
            put_pair(hi_ref, lo_ref, k0 * 128 + k1 * 8, out[k1], out[k1 + 1])
        return 0
    lax.fori_loop(0, 16, body, 0)

def dot3(hi, lo, whi, wlo):
    d = functools.partial(jnp.dot, preferred_element_type=f32)
    return d(hi, whi) + d(lo, whi) + d(hi, wlo)

def ahead_part(i, hi_ref, lo_ref, q, mats, chunk):
    rows = pl.ds(pl.multiple_of(i * chunk, chunk), chunk)
    q[rows, :] = dot3(hi_ref[rows, :], lo_ref[rows, :], mats[0], mats[1])

def ahead(hi_ref, lo_ref, q, mats, chunk=1024):
    def body(i, _):
        ahead_part(i, hi_ref, lo_ref, q, mats, chunk)
        return 0
    lax.fori_loop(0, 2048 // chunk, body, 0)

def weigh_back(i, q, resp, mats, chunk):
    rows = pl.ds(pl.multiple_of(i * chunk, chunk), chunk)
    p = cmul((q[rows, 0:128], q[rows, 128:256]), resp[0, rows, :], resp[1, rows, :])
    hi, lo = split(jnp.concatenate(p, axis=1))
    q[rows, :] = dot3(hi, lo, mats[2], mats[3])

def stage_k1(k0, q, y, tab):
    v = []
    for k1 in range(16):
        rows = pl.ds(pl.multiple_of(k0 * 128 + k1 * 8, 8), 8)
        row = pl.ds(k0 + 16 * k1, 1)
        v.append(cmulc((q[rows, 0:128], q[rows, 128:256]), tab[0, row, :], tab[1, row, :]))
    for m1, a in enumerate(dft16(v, 1)):
        y[0, k0 * 16 + m1], y[1, k0 * 16 + m1] = a

def stage_k0(y, out, tab, flip, g):
    def body(m1, _):
        v = []
        for k0 in range(16):
            a = (y[0, k0 * 16 + m1], y[1, k0 * 16 + m1])
            if k0:
                row = pl.ds(m1 * 16 + k0, 1)
                a = cmulc(a, tab[2, row, :], tab[3, row, :])
            v.append(a)
        for j, a in enumerate(half16(v, 1, flip)):
            lanes = pl.ds(pl.multiple_of(j * 2048 + m1 * 128, 128), 128)
            rows = pl.ds(pl.multiple_of(8 * g, 8), 8)
            out[0, rows, lanes], out[1, rows, lanes] = a
        return 0
    lax.fori_loop(0, 16, body, 0)

def phase(idx):
    idx = (idx & (N - 1))
    idx = jnp.where(idx >= N // 2, idx - N, idx)
    ang = idx.astype(f32) * (2 * math.pi / N)
    return jnp.cos(ang), -jnp.sin(ang)

def response(line, r, bank, slabs, shifts, resp):
    sub = lax.broadcasted_iota(jnp.int32, (8, 128), 0)
    lane = lax.broadcasted_iota(jnp.int32, (8, 128), 1)
    sl, sh = slabs[line], shifts[line]
    e = [phase((16 * (sub + 8 * h) + 256 * lane) * sh) for h in range(2)]
    w = phase(jnp.full((8, 128), 1, jnp.int32) * sh)
    for i in range(16):
        hr = bank[0, sl, 16 * i:16 * i + 16, :].astype(f32)
        hi = bank[1, sl, 16 * i:16 * i + 16, :].astype(f32)
        for h in range(2):
            o = cmul((hr[8 * h:8 * h + 8], hi[8 * h:8 * h + 8]), *e[h])
            rows = pl.ds((16 * i + 8 * h) * 8 + r, 8, stride=8)
            resp[0, rows, :] = o[0]
            resp[1, rows, :] = o[1]
        if i < 15:
            e = [cmul(x, *w) for x in e]


def place_filters(raw, lines, turned, bank, part, chunk):
    def spread(i, _):
        lanes = pl.ds(pl.multiple_of(i * 2048, 2048), 2048)
        block = raw[:, lanes].astype(f32)
        for t in range(16):
            for slab in range(2):
                lines[slab, pl.ds(i * 16 + t, 1), :] = block[slab:slab + 1, 128 * t:128 * t + 128]
        return 0
    lax.fori_loop(0, 16, spread, 0)
    for slab in range(2):
        for h in range(2):
            flat = jnp.transpose(lines[slab, pl.ds(h, 128, stride=2), :])
            for b in range(8):
                turned[slab, pl.ds(8 * h + b, 16, stride=16), :] = flat[16 * b:16 * b + 16]
        bank[part, 2 * chunk + slab] = turned[slab].astype(bf16)


def kernel(
    echoes, filters, slabs, shifts, mats_h, tab_h, out,
    xs, est, bank, raw, lines, turned, mats, tab, y, ahi, alo, q0, q1, resp0, resp1,
    loc, es, er, fs, fr, zs, zr, cs, cr,
):
    t, b, s = (lax.axis_index(n) for n in ("turn", "blk", "strip"))
    yy, core = t // 2, t % 2
    xlo, z = b // 8, b % 8
    xx = 2 * s + xlo

    def at_y(dy, dc):
        return (((yy + dy) % 4) * 2 + (core + dc) % 2, b, s)

    def at_x(d):
        x = (xx + d) % 4
        return (t, (x % 2) * 8 + z, x // 2)

    def at_z(d):
        return (t, xlo * 8 + (z + d) % 8, s)

    mate, twin = at_y(0, 1), (t, b, 1 - s)
    peers = [at_y(dy, dc) for dy, dc in ((0, 1), (1, 0), (3, 0), (1, 1), (3, 1), (2, 0), (2, 1))]

    barrier = pltpu.get_barrier_semaphore()
    known = peers + [twin, at_x(1), at_x(3), at_z(1), at_z(7)]
    for d in known:
        pl.semaphore_signal(barrier, inc=1, device_id=d, device_id_type=MESH)

    mine = 2 * t + s
    local = [
        pltpu.make_async_copy(filters.at[core], raw, loc.at[0]),
        pltpu.make_async_copy(echoes, est, loc.at[1]),
        pltpu.make_async_copy(echoes.at[:, t, 0], xs.at[0, mine], loc.at[2]),
        pltpu.make_async_copy(echoes.at[:, t, 1], xs.at[1, mine], loc.at[3]),
        pltpu.make_async_copy(mats_h, mats, loc.at[4]),
        pltpu.make_async_copy(tab_h, tab, loc.at[5]),
    ]
    for c in local:
        c.start()
    local[0].wait()
    place_filters(raw, lines, turned, bank, core, b)
    for c in local[1:]:
        c.wait()
    pl.semaphore_wait(barrier, len(known))

    sent = []

    def send(src, dst, ssem, rsem, device):
        c = pltpu.make_async_remote_copy(
            src, dst, ssem, rsem, device_id=device, device_id_type=MESH
        )
        c.start()
        sent.append(c)

    def arrived(ref, ssem, rsem):
        pltpu.make_async_remote_copy(
            ref, ref, ssem, rsem, device_id=twin, device_id_type=MESH
        ).wait_recv()

    def slot(device):
        return 2 * device[0] + s

    def forward(g, j):
        ref = xs.at[g, j]
        send(ref, ref, es.at[g, j], er.at[g, j], twin)

    def echo(g, device):
        j = slot(device)
        arrived(xs.at[g, j], es.at[g, j], er.at[g, j])
        forward(g, j)

    def slab(part, n, d):
        side = xlo if n < 2 else 1 - xlo
        return bank.at[part, 2 * (side * 8 + (z + d) % 8) + n % 2]

    def over_z(n, hop, way):
        ref = slab(core, n, (1 - hop if way == 0 else hop - 1) % 8)
        send(ref, ref, zs.at[way, hop - 1, n], zr.at[way, hop - 1, n], at_z(1 if way == 0 else 7))

    def over_core(n, d):
        ref = slab(core, n, d)
        send(ref, ref, cs.at[n, d], cr.at[n, d], mate)

    def relay(u, hop):
        for i in range(2):
            n = 2 * u + i
            for way in range(2):
                if hop == 4 and way != i:
                    continue
                d = (-hop if way == 0 else hop) % 8
                arrived(slab(core, n, d), zs.at[way, hop - 1, n], zr.at[way, hop - 1, n])
                if hop < 3 or (hop == 3 and way == i):
                    over_z(n, hop + 1, way)
                over_core(n, d)

    def own_filters():
        for i, d in ((0, 1), (1, 3)):
            ref = slab(core, i, 0)
            send(ref, ref, fs.at[i], fr.at[i], at_x(d))
        for i in range(2):
            over_z(i, 1, 0)
            over_z(i, 1, 1)

    def other_filters():
        for i in range(2):
            arrived(slab(core, 2 + i, 0), fs.at[i], fr.at[i])
            over_z(2 + i, 1, 0)
            over_z(2 + i, 1, 1)
            over_core(2 + i, 0)

    def over_y(g):
        for k, d in enumerate(peers):
            send(est.at[:, d[0], g], xs.at[g, mine], loc.at[8 + 8 * g + k], er.at[g, mine], d)

    def echoes_in(g):
        for k in range(8):
            j = 2 * k + 1 - s
            arrived(xs.at[g, j], es.at[g, j], er.at[g, j])

    def filters_in():
        for n in range(4):
            for d in range(8):
                arrived(slab(1 - core, n, d), cs.at[n, d], cr.at[n, d])

    flip = 1.0 - 2.0 * s.astype(f32)

    own_filters()
    forward(0, mine)
    over_y(0)
    for i in range(2): over_core(i, 0)
    echo(0, peers[0])
    forward(1, mine)
    other_filters()
    for d in peers[1:3]: echo(0, d)
    relay(0, 1)
    for d in peers[3:5]: echo(0, d)
    relay(1, 1)
    over_y(1)
    for d in peers[5:]: echo(0, d)
    echo(1, peers[0])
    relay(0, 2)
    for d in peers[1:3]: echo(1, d)
    relay(1, 2)
    for d in peers[3:5]: echo(1, d)
    for d in peers[5:]: echo(1, d)
    relay(0, 3)

    echoes_in(0)
    stage_j(xs.at[0], y, tab)
    relay(1, 3)
    stage_m(y, ahi, alo, tab)
    relay(0, 4)
    ahead(ahi, alo, q0, mats)
    relay(1, 4)

    echoes_in(1)
    stage_j(xs.at[1], y, tab)
    stage_m(y, ahi, alo, tab)
    filters_in()

    def shape(i, _):
        ahead_part(i, ahi, alo, q1, mats, 512)
        for half in range(2):
            response(2 * i + half, 2 * i + half, bank, slabs, shifts, resp0)
            response(8 + 2 * i + half, 2 * i + half, bank, slabs, shifts, resp1)
        return 0

    lax.fori_loop(0, 4, shape, 0)

    def first(i, _):
        weigh_back(i, q0, resp0, mats, 1024)
        return 0

    lax.fori_loop(0, 2, first, 0)

    def second(i, _):
        weigh_back(i, q1, resp1, mats, 512)
        for n in range(4):
            stage_k1(4 * i + n, q0, y, tab)
        return 0

    lax.fori_loop(0, 4, second, 0)
    stage_k0(y, out, tab, flip, 0)

    def last(k0, _):
        stage_k1(k0, q1, y, tab)
        return 0

    lax.fori_loop(0, 16, last, 0)
    stage_k0(y, out, tab, flip, 1)
    for c in sent:
        c.wait_send()


def per_device(echoes, filters, slab_index, shifts):
    mats, tab = tables()
    hbm = pl.BlockSpec(memory_space=pl.ANY)
    smem = pl.BlockSpec(memory_space=pltpu.SMEM)
    dma = pltpu.SemaphoreType.DMA
    return pl.pallas_call(
        kernel,
        out_shape=pltpu.VMEM((2, 16, N // 2), f32),
        in_specs=[hbm, hbm, smem, smem, hbm, hbm],
        out_specs=pl.BlockSpec(memory_space=pltpu.VMEM),
        scratch_shapes=[
            pltpu.VMEM((2, 16, 2, 8, 2048), bf16),
            pltpu.VMEM((2, 8, 2, 8, 2048), bf16),
            pltpu.VMEM((2, 32, 256, 128), bf16),
            pltpu.VMEM((2, N), bf16),
            pltpu.VMEM((2, 256, 128), f32),
            pltpu.VMEM((2, 256, 128), f32),
            pltpu.VMEM((4, 256, 256), bf16),
            pltpu.VMEM((4, 256, 128), f32),
            pltpu.VMEM((2, 256, 8, 128), f32),
            pltpu.VMEM((2048, 256), bf16),
            pltpu.VMEM((2048, 256), bf16),
            pltpu.VMEM((2048, 256), f32),
            pltpu.VMEM((2048, 256), f32),
            pltpu.VMEM((2, 2048, 128), f32),
            pltpu.VMEM((2, 2048, 128), f32),
            dma((24,)),
            dma((2, 16)),
            dma((2, 16)),
            dma((2,)),
            dma((2,)),
            dma((2, 4, 4)),
            dma((2, 4, 4)),
            dma((4, 8)),
            dma((4, 8)),
        ],
        compiler_params=pltpu.CompilerParams(
            collective_id=0, has_side_effects=True, vmem_limit_bytes=64946176
        ),
    )(
        echoes.reshape(2, 8, 2, 8, 2048), filters, slab_index, shifts,
        jnp.asarray(mats), jnp.asarray(tab),
    )


def solution(mesh):
    in_specs = (
        P(None, "blk", ("turn", "strip")),
        P(None, "blk", None),
        P(("blk", "turn")),
        P(("blk", "turn")),
    )
    out_specs = P(None, ("blk", "turn"), "strip")
    return jax.shard_map(
        per_device, mesh=mesh, in_specs=in_specs, out_specs=out_specs, check_vma=False
    )
```

```python
import functools
import math

import numpy as np
import jax
import jax.numpy as jnp
from jax import lax
from jax.experimental import pallas as pl
from jax.experimental.pallas import tpu as pltpu
from jax.sharding import PartitionSpec as P

N = 32768
f32, bf16 = jnp.float32, jnp.bfloat16
MESH = pl.DeviceIdType.MESH

def cis(phase, length, sign):
    ang = (np.asarray(phase, np.int64) % length).astype(np.float64) * (2 * np.pi / length)
    return np.cos(ang), sign * np.sin(ang)

def halves(mat):
    hi = mat.astype(np.float32).astype(bf16)
    lo = (mat - hi.astype(np.float64)).astype(np.float32).astype(bf16)
    return hi, lo

def tables():
    lane = np.arange(128)
    c, s = cis(np.outer(lane, lane), 128, -1)
    fwd = np.block([[c, s], [-s, c]])
    inv = np.block([[c, -s], [s, c]]) / N
    mats = np.stack([*halves(fwd), *halves(inv)])
    tile = np.arange(256)
    tw = np.stack(cis(np.outer(tile, lane), N, -1)).astype(np.float32)
    ij = np.outer(np.arange(16), np.arange(16)).reshape(256, 1) * np.ones((1, 128), np.int64)
    ct = np.stack(cis(ij, 256, -1)).astype(np.float32)
    return mats, np.concatenate([tw, ct])

R2 = math.sqrt(0.5)
C1, S1 = math.cos(math.pi / 8), math.sin(math.pi / 8)

def cadd(a, b): return (a[0] + b[0], a[1] + b[1])
def csub(a, b): return (a[0] - b[0], a[1] - b[1])

def turn16(a, p, sign):
    p = (sign * p) % 16
    q, r = divmod(p, 4)
    x, y = a
    if r == 2:
        x, y = ((x - y) * R2, (x + y) * R2)
    elif r:
        c, s = (C1, S1) if r == 1 else (S1, C1)
        x, y = (x * c - y * s, x * s + y * c)
    return [(x, y), (-y, x), (-x, -y), (y, -x)][q]

def fold4(a, b, c, d, sign):
    e, f, g, h = cadd(a, c), csub(a, c), cadd(b, d), csub(b, d)
    if sign > 0:
        t, u = (f[0] - h[1], f[1] + h[0]), (f[0] + h[1], f[1] - h[0])
    else:
        t, u = (f[0] + h[1], f[1] - h[0]), (f[0] - h[1], f[1] + h[0])
    return cadd(e, g), t, csub(e, g), u

def dft16(v, sign):
    cols = [fold4(v[b], v[b + 4], v[b + 8], v[b + 12], sign) for b in range(4)]
    out = [None] * 16
    for a in range(4):
        o = fold4(*[turn16(cols[b][a], a * b, sign) for b in range(4)], sign)
        for c in range(4):
            out[a + 4 * c] = o[c]
    return out

def dft8(v, sign):
    even = fold4(v[0], v[2], v[4], v[6], sign)
    odd = fold4(v[1], v[3], v[5], v[7], sign)
    odd = [turn16(o, 2 * i, sign) for i, o in enumerate(odd)]
    return [cadd(e, o) for e, o in zip(even, odd)] + [csub(e, o) for e, o in zip(even, odd)]

def half16(v, sign, flip):
    even = dft8(v[0::2], sign)
    odd = dft8([(flip * a, flip * b) for a, b in v[1::2]], sign)
    return [cadd(e, turn16(o, i, sign)) for i, (e, o) in enumerate(zip(even, odd))]

def cmul(a, c, s): return (a[0] * c - a[1] * s, a[0] * s + a[1] * c)
def cmulc(a, c, s): return (a[0] * c + a[1] * s, a[1] * c - a[0] * s)

def split(x):
    hi = x.astype(bf16)
    return hi, (x - hi.astype(f32)).astype(bf16)

def stage_j(xs, y, tab):
    def body(m1, _):
        lanes = pl.ds(pl.multiple_of(m1 * 128, 128), 128)
        v = [(xs[j, 0, :, lanes].astype(f32), xs[j, 1, :, lanes].astype(f32)) for j in range(16)]
        for k0, a in enumerate(dft16(v, -1)):
            if k0:
                row = pl.ds(m1 * 16 + k0, 1)
                a = cmul(a, tab[2, row, :], tab[3, row, :])
            y[0, k0 * 16 + m1], y[1, k0 * 16 + m1] = a
        return 0
    lax.fori_loop(0, 16, body, 0)

def put_pair(hi_ref, lo_ref, row, a, b):
    rows = pl.ds(pl.multiple_of(row, 16), 16)
    for part, lanes in ((0, slice(0, 128)), (1, slice(128, 256))):
        hi, lo = split(jnp.concatenate([a[part], b[part]], axis=0))
        hi_ref[rows, lanes] = hi
        lo_ref[rows, lanes] = lo

def stage_m(y, hi_ref, lo_ref, tab):
    def body(k0, _):
        out = dft16([(y[0, k0 * 16 + m1], y[1, k0 * 16 + m1]) for m1 in range(16)], -1)
        out = [cmul(a, tab[0, pl.ds(k0 + 16 * k1, 1), :], tab[1, pl.ds(k0 + 16 * k1, 1), :]) for k1, a in enumerate(out)]
        for k1 in range(0, 16, 2):
            put_pair(hi_ref, lo_ref, k0 * 128 + k1 * 8, out[k1], out[k1 + 1])
        return 0
    lax.fori_loop(0, 16, body, 0)

def dot3(hi, lo, whi, wlo):
    d = functools.partial(jnp.dot, preferred_element_type=f32)
    return d(hi, whi) + d(lo, whi) + d(hi, wlo)

def ahead_part(i, hi_ref, lo_ref, q, mats, chunk):
    rows = pl.ds(pl.multiple_of(i * chunk, chunk), chunk)
    q[rows, :] = dot3(hi_ref[rows, :], lo_ref[rows, :], mats[0], mats[1])

def ahead(hi_ref, lo_ref, q, mats, chunk=1024):
    def body(i, _):
        ahead_part(i, hi_ref, lo_ref, q, mats, chunk)
        return 0
    lax.fori_loop(0, 2048 // chunk, body, 0)

def weigh_back(i, q, resp, mats, chunk):
    rows = pl.ds(pl.multiple_of(i * chunk, chunk), chunk)
    p = cmul((q[rows, 0:128], q[rows, 128:256]), resp[0, rows, :], resp[1, rows, :])
    hi, lo = split(jnp.concatenate(p, axis=1))
    q[rows, :] = dot3(hi, lo, mats[2], mats[3])

def stage_k1(k0, q, y, tab):
    v = []
    for k1 in range(16):
        rows = pl.ds(pl.multiple_of(k0 * 128 + k1 * 8, 8), 8)
        row = pl.ds(k0 + 16 * k1, 1)
        v.append(cmulc((q[rows, 0:128], q[rows, 128:256]), tab[0, row, :], tab[1, row, :]))
    for m1, a in enumerate(dft16(v, 1)):
        y[0, k0 * 16 + m1], y[1, k0 * 16 + m1] = a

def stage_k0(y, out, tab, flip, g):
    def body(m1, _):
        v = []
        for k0 in range(16):
            a = (y[0, k0 * 16 + m1], y[1, k0 * 16 + m1])
            if k0:
                row = pl.ds(m1 * 16 + k0, 1)
                a = cmulc(a, tab[2, row, :], tab[3, row, :])
            v.append(a)
        for j, a in enumerate(half16(v, 1, flip)):
            lanes = pl.ds(pl.multiple_of(j * 2048 + m1 * 128, 128), 128)
            rows = pl.ds(pl.multiple_of(8 * g, 8), 8)
            out[0, rows, lanes], out[1, rows, lanes] = a
        return 0
    lax.fori_loop(0, 16, body, 0)

def phase(idx):
    idx = (idx & (N - 1))
    idx = jnp.where(idx >= N // 2, idx - N, idx)
    ang = idx.astype(f32) * (2 * math.pi / N)
    return jnp.cos(ang), -jnp.sin(ang)

def response(line, r, bank, slabs, shifts, resp):
    sub = lax.broadcasted_iota(jnp.int32, (8, 128), 0)
    lane = lax.broadcasted_iota(jnp.int32, (8, 128), 1)
    sl, sh = slabs[line], shifts[line]
    e = [phase((16 * (sub + 8 * h) + 256 * lane) * sh) for h in range(2)]
    w = phase(jnp.full((8, 128), 1, jnp.int32) * sh)
    for i in range(16):
        hr = bank[0, sl, 16 * i:16 * i + 16, :].astype(f32)
        hi = bank[1, sl, 16 * i:16 * i + 16, :].astype(f32)
        for h in range(2):
            o = cmul((hr[8 * h:8 * h + 8], hi[8 * h:8 * h + 8]), *e[h])
            rows = pl.ds((16 * i + 8 * h) * 8 + r, 8, stride=8)
            resp[0, rows, :] = o[0]
            resp[1, rows, :] = o[1]
        if i < 15:
            e = [cmul(x, *w) for x in e]


def place_filters(raw, lines, turned, bank, part, chunk):
    def spread(i, _):
        lanes = pl.ds(pl.multiple_of(i * 2048, 2048), 2048)
        block = raw[:, lanes].astype(f32)
        for t in range(16):
            for slab in range(2):
                lines[slab, pl.ds(i * 16 + t, 1), :] = block[slab:slab + 1, 128 * t:128 * t + 128]
        return 0
    lax.fori_loop(0, 16, spread, 0)
    for slab in range(2):
        for h in range(2):
            flat = jnp.transpose(lines[slab, pl.ds(h, 128, stride=2), :])
            for b in range(8):
                turned[slab, pl.ds(8 * h + b, 16, stride=16), :] = flat[16 * b:16 * b + 16]
        bank[part, 2 * chunk + slab] = turned[slab].astype(bf16)


def kernel(
    echoes, filters, slabs, shifts, mats_h, tab_h, out,
    xs, est, bank, raw, lines, turned, mats, tab, y, ahi, alo, q0, q1, resp0, resp1,
    loc, es, er, fs, fr, zs, zr, cs, cr,
):
    t, b, s = (lax.axis_index(n) for n in ("turn", "blk", "strip"))
    yy, core = t // 2, t % 2
    xlo, z = b // 8, b % 8
    xx = 2 * s + xlo

    def at_y(dy, dc):
        return (((yy + dy) % 4) * 2 + (core + dc) % 2, b, s)

    def at_x(d):
        x = (xx + d) % 4
        return (t, (x % 2) * 8 + z, x // 2)

    def at_z(d):
        return (t, xlo * 8 + (z + d) % 8, s)

    mate, twin = at_y(0, 1), (t, b, 1 - s)
    peers = [at_y(dy, dc) for dy, dc in ((0, 1), (1, 0), (3, 0), (1, 1), (3, 1), (2, 0), (2, 1))]

    barrier = pltpu.get_barrier_semaphore()
    known = peers + [twin, at_x(1), at_x(3), at_z(1), at_z(7)]
    for d in known:
        pl.semaphore_signal(barrier, inc=1, device_id=d, device_id_type=MESH)

    mine = 2 * t + s
    local = [
        pltpu.make_async_copy(filters.at[core], raw, loc.at[0]),
        pltpu.make_async_copy(echoes, est, loc.at[1]),
        pltpu.make_async_copy(echoes.at[:, t, 0], xs.at[0, mine], loc.at[2]),
        pltpu.make_async_copy(echoes.at[:, t, 1], xs.at[1, mine], loc.at[3]),
        pltpu.make_async_copy(mats_h, mats, loc.at[4]),
        pltpu.make_async_copy(tab_h, tab, loc.at[5]),
    ]
    for c in local:
        c.start()
    local[0].wait()
    place_filters(raw, lines, turned, bank, core, b)
    for c in local[1:]:
        c.wait()
    pl.semaphore_wait(barrier, len(known))

    sent = []

    def send(src, dst, ssem, rsem, device):
        c = pltpu.make_async_remote_copy(
            src, dst, ssem, rsem, device_id=device, device_id_type=MESH
        )
        c.start()
        sent.append(c)

    def arrived(ref, ssem, rsem):
        pltpu.make_async_remote_copy(
            ref, ref, ssem, rsem, device_id=twin, device_id_type=MESH
        ).wait_recv()

    def slot(device):
        return 2 * device[0] + s

    def forward(g, j):
        ref = xs.at[g, j]
        send(ref, ref, es.at[g, j], er.at[g, j], twin)

    def echo(g, device):
        j = slot(device)
        arrived(xs.at[g, j], es.at[g, j], er.at[g, j])
        forward(g, j)

    def slab(part, n, d):
        side = xlo if n < 2 else 1 - xlo
        return bank.at[part, 2 * (side * 8 + (z + d) % 8) + n % 2]

    def over_z(n, hop, way):
        ref = slab(core, n, (1 - hop if way == 0 else hop - 1) % 8)
        send(ref, ref, zs.at[way, hop - 1, n], zr.at[way, hop - 1, n], at_z(1 if way == 0 else 7))

    def over_core(n, d):
        ref = slab(core, n, d)
        send(ref, ref, cs.at[n, d], cr.at[n, d], mate)

    def relay(u, hop):
        for i in range(2):
            n = 2 * u + i
            for way in range(2):
                if hop == 4 and way != i:
                    continue
                d = (-hop if way == 0 else hop) % 8
                arrived(slab(core, n, d), zs.at[way, hop - 1, n], zr.at[way, hop - 1, n])
                if hop < 3 or (hop == 3 and way == i):
                    over_z(n, hop + 1, way)
                over_core(n, d)

    def own_filters():
        for i, d in ((0, 1), (1, 3)):
            ref = slab(core, i, 0)
            send(ref, ref, fs.at[i], fr.at[i], at_x(d))
        for i in range(2):
            over_z(i, 1, 0)
            over_z(i, 1, 1)

    def other_filters():
        for i in range(2):
            arrived(slab(core, 2 + i, 0), fs.at[i], fr.at[i])
            over_z(2 + i, 1, 0)
            over_z(2 + i, 1, 1)
            over_core(2 + i, 0)

    def over_y(g):
        for k, d in enumerate(peers):
            send(est.at[:, d[0], g], xs.at[g, mine], loc.at[8 + 8 * g + k], er.at[g, mine], d)

    def echoes_in(g):
        for k in range(8):
            j = 2 * k + 1 - s
            arrived(xs.at[g, j], es.at[g, j], er.at[g, j])

    def filters_in():
        for n in range(4):
            for d in range(8):
                arrived(slab(1 - core, n, d), cs.at[n, d], cr.at[n, d])

    flip = 1.0 - 2.0 * s.astype(f32)

    own_filters()
    forward(0, mine)
    over_y(0)
    for i in range(2): over_core(i, 0)
    echo(0, peers[0])
    other_filters()
    for d in peers[1:3]: echo(0, d)
    relay(0, 1)
    for d in peers[3:5]: echo(0, d)
    relay(1, 1)
    for d in peers[5:]: echo(0, d)
    forward(1, mine)
    over_y(1)
    echo(1, peers[0])
    relay(0, 2)
    for d in peers[1:3]: echo(1, d)
    relay(1, 2)
    for d in peers[3:5]: echo(1, d)
    for d in peers[5:]: echo(1, d)
    relay(0, 3)

    echoes_in(0)
    stage_j(xs.at[0], y, tab)
    relay(1, 3)
    stage_m(y, ahi, alo, tab)
    relay(0, 4)
    ahead(ahi, alo, q0, mats)
    relay(1, 4)

    echoes_in(1)
    stage_j(xs.at[1], y, tab)
    stage_m(y, ahi, alo, tab)
    filters_in()

    def shape(i, _):
        ahead_part(i, ahi, alo, q1, mats, 512)
        for half in range(2):
            response(2 * i + half, 2 * i + half, bank, slabs, shifts, resp0)
            response(8 + 2 * i + half, 2 * i + half, bank, slabs, shifts, resp1)
        return 0

    lax.fori_loop(0, 4, shape, 0)

    def first(i, _):
        weigh_back(i, q0, resp0, mats, 512)
        return 0

    lax.fori_loop(0, 4, first, 0)

    def second(i, _):
        weigh_back(i, q1, resp1, mats, 512)
        for n in range(4):
            stage_k1(4 * i + n, q0, y, tab)
        return 0

    lax.fori_loop(0, 4, second, 0)
    stage_k0(y, out, tab, flip, 0)

    def last(k0, _):
        stage_k1(k0, q1, y, tab)
        return 0

    lax.fori_loop(0, 16, last, 0)
    stage_k0(y, out, tab, flip, 1)
    for c in sent:
        c.wait_send()


def per_device(echoes, filters, slab_index, shifts):
    mats, tab = tables()
    hbm = pl.BlockSpec(memory_space=pl.ANY)
    smem = pl.BlockSpec(memory_space=pltpu.SMEM)
    dma = pltpu.SemaphoreType.DMA
    return pl.pallas_call(
        kernel,
        out_shape=pltpu.VMEM((2, 16, N // 2), f32),
        in_specs=[hbm, hbm, smem, smem, hbm, hbm],
        out_specs=pl.BlockSpec(memory_space=pltpu.VMEM),
        scratch_shapes=[
            pltpu.VMEM((2, 16, 2, 8, 2048), bf16),
            pltpu.VMEM((2, 8, 2, 8, 2048), bf16),
            pltpu.VMEM((2, 32, 256, 128), bf16),
            pltpu.VMEM((2, N), bf16),
            pltpu.VMEM((2, 256, 128), f32),
            pltpu.VMEM((2, 256, 128), f32),
            pltpu.VMEM((4, 256, 256), bf16),
            pltpu.VMEM((4, 256, 128), f32),
            pltpu.VMEM((2, 256, 8, 128), f32),
            pltpu.VMEM((2048, 256), bf16),
            pltpu.VMEM((2048, 256), bf16),
            pltpu.VMEM((2048, 256), f32),
            pltpu.VMEM((2048, 256), f32),
            pltpu.VMEM((2, 2048, 128), f32),
            pltpu.VMEM((2, 2048, 128), f32),
            dma((24,)),
            dma((2, 16)),
            dma((2, 16)),
            dma((2,)),
            dma((2,)),
            dma((2, 4, 4)),
            dma((2, 4, 4)),
            dma((4, 8)),
            dma((4, 8)),
        ],
        compiler_params=pltpu.CompilerParams(
            collective_id=0, has_side_effects=True, vmem_limit_bytes=64946176
        ),
    )(
        echoes.reshape(2, 8, 2, 8, 2048), filters, slab_index, shifts,
        jnp.asarray(mats), jnp.asarray(tab),
    )


def solution(mesh):
    in_specs = (
        P(None, "blk", ("turn", "strip")),
        P(None, "blk", None),
        P(("blk", "turn")),
        P(("blk", "turn")),
    )
    out_specs = P(None, ("blk", "turn"), "strip")
    return jax.shard_map(
        per_device, mesh=mesh, in_specs=in_specs, out_specs=out_specs, check_vma=False
    )
```
